32 devices in a mesh: ep: 16 (over z, y, x), tp: 2 (over core).
Axes of the slice: x: 2, y: 2, z: 4, core: 2. Of those that a mesh axis runs over, the one named last changes fastest.
Arguments:
- tokens: bfloat16 [512, 6144], P('ep', 'tp'), may hold values from -6 to 6
- expert_ids: int32 [512, 8], P('ep'), may hold values from 0 to 15, all different within a row; in each aligned block of 32 rows (0 to 31, 32 to 63, ...) at most 30 rows name the same one
- gate_scores: float32 [512, 8], P('ep'), may hold values from 0.05 to 0.6
- routed_gate: bfloat16 [16, 6144, 2048], P('ep', None, 'tp'), may hold values from -0.078125 to 0.078125
- routed_up: bfloat16 [16, 6144, 2048], P('ep', None, 'tp'), may hold values from -0.078125 to 0.078125
- routed_down: bfloat16 [16, 2048, 6144], P('ep', 'tp'), may hold values from -0.1875 to 0.1875
- shared_gate: bfloat16 [6144, 2048], P(None, 'tp'), may hold values from -0.078125 to 0.078125
- shared_up: bfloat16 [6144, 2048], P(None, 'tp'), may hold values from -0.078125 to 0.078125
- shared_down: bfloat16 [2048, 6144], P('tp'), may hold values from -0.1875 to 0.1875
Outputs:
- moe_out: bfloat16 [512, 6144], P('ep', 'tp')
The draws below stay inside these ranges and needn't reach their ends.
Inputs may be any that keep to these rules, and one draw needn't show every extreme that they name: `expert_ids`: each row names 8 different experts. Among the 32 rows of one aligned block no expert is named more than 30 times, and in some block one expert is named exactly 30 times.
All inputs are finite; a program needn't handle non-finite values.
Results may differ from the reference program's by a relative error of at most 0.019.
Values may be sent and summed in bfloat16 or wider, within the bound.
A program may use at most 128 MiB of HBM per device.

```python
import math
import jax
import jax.numpy as jnp
import numpy as np
from jax import lax

D = 6144
FF = 2048
FF_S = 2048
TOPK = 8
TOK_EP = 32
EXPERTS = 16
C = 30
TOKENS = 512
N_EP = 16
N_TP = 2


def raised(result, own_key, source, target, shards_of, factor):
    def block_of(axis_at):
        return (jnp.arange(result.shape[axis_at]) // (result.shape[axis_at] // shards_of)).reshape((-1,) + (1,) * (result.ndim - 1 - axis_at))

    one_side = jax.random.permutation(own_key, shards_of)[block_of(target)]
    second = (block_of(target) + shards_of // 2) % shards_of
    return jnp.where((block_of(source) == one_side) | (block_of(source) == second), factor * result, result)


def block_levels(rng, dims, cuts, smallest, high):
    loudness, own = 1.0, jax.random.fold_in(rng, 6)
    for dim, blocks in cuts:
        steps = jnp.exp(jax.random.uniform(jax.random.fold_in(own, dim), (blocks,), jnp.float32, smallest / len(cuts), high / len(cuts)))
        loudness = loudness * jnp.repeat(steps, dims[dim] // blocks).reshape([-1 if axis == dim else 1 for axis in range(len(dims))])
    return loudness


def assign_block(own_key, own, number, rows, count, top, reach, slope):
    sequence = jax.random.permutation(own_key, count)
    crowded, common = portions_of(count, rows * top, reach, slope, True), portions_of(count, rows * top, reach, slope, False)
    places = jnp.arange(count)

    def named(tallies, rotation):
        used = int((tallies > 0).sum())
        fixed = max(1, used // 4)
        moved = fixed + (places - fixed + rotation * (used - fixed)) % max(1, count - fixed)
        return jnp.zeros((count,), jnp.int32).at[sequence[jnp.where(places < fixed, places, moved)]].set(jnp.asarray(tallies, jnp.int32))

    tallies = jnp.where(number % 4 == 0, named(crowded, number // 4), named(common, number - number // 4 - 1))
    mixed = jax.random.permutation(jax.random.fold_in(own, 3), count)
    source_of, receiver = mixed[0:count // 2 * 2:2], mixed[1:count // 2 * 2:2]
    room = jnp.minimum(tallies[source_of] - 1, reach - tallies[receiver]) // 2
    room = jnp.where((source_of == sequence[0]) | (receiver == sequence[0]) | (tallies[receiver] == 0), 0, jnp.maximum(room, 0))
    moved = jax.random.randint(jax.random.fold_in(own, 4), (count // 2,), 0, 1 << 20) % (room + 1)
    tallies = tallies.at[source_of].add(-moved).at[receiver].add(moved)
    items = jnp.searchsorted(jnp.cumsum(tallies), jnp.arange(rows * top), side="right").astype(jnp.int32)
    table = items.reshape(top, rows).T
    table = table[jax.random.permutation(jax.random.fold_in(own, 1), rows)]
    rotation = jax.random.randint(jax.random.fold_in(own, 2), (rows, 1), 0, top)
    return jnp.take_along_axis(table, (jnp.arange(top)[None, :] + rotation) % top, axis=1)


def portions_of(amount, total, bound, slope, full):
    weights = [(1 << 20) // math.isqrt(grade ** slope) + 1 for grade in range(1, amount + 1)]
    largest = bound if full else min(bound, max(-(-total // amount), total * weights[0] // sum(weights)))
    least = 1 if total - largest >= amount - 1 else 0
    holding, surplus = [largest] + [least] * (amount - 1), total - largest - least * (amount - 1)
    while surplus > 0:
        candidates = [i for i in range(1, amount) if holding[i] < largest] or [i for i in range(1, amount) if holding[i] < bound]
        pool, budget = sum([weights[i] for i in candidates]), surplus
        for i in candidates:
            extra = min(bound - holding[i], max(1, budget * weights[i] // pool), surplus)
            holding[i] = holding[i] + extra
            surplus = surplus - extra
    return np.array(holding)


def bell_draw(own_key, dims, deviation, reach, cuts=(), kind=jnp.bfloat16):
    values = jax.random.normal(own_key, dims, jnp.float32) * deviation
    if len(cuts) > 0:
        values = block_levels(own_key, dims, cuts, -0.22, 0.18) * values
    return jnp.clip(values, min=-reach, max=reach).astype(kind)


def noise_with(stream_key, extent, scale, limit, cuts, heavy, held_as=jnp.bfloat16):
    array = scale * jax.random.normal(stream_key, extent, jnp.float32)
    if cuts:
        array = array * block_levels(stream_key, extent, cuts, -0.22, 0.18)
    return jnp.clip(raised(array, jax.random.fold_in(stream_key, 3), *heavy), -limit, limit).astype(held_as)


def setup_inputs(seed: int = 0) -> dict:
    key_list = jax.random.split(jax.random.key(seed), 10)
    tokens = bell_draw(key_list[0], (TOKENS, D), 1.0, 6.0, ((0, 16), (1, 2)))
    expert_ids_keys = jax.random.split(jax.random.fold_in(key_list[1], 1), TOKENS // TOK_EP)
    expert_ids_turns = jax.random.permutation(jax.random.fold_in(key_list[1], 3), TOKENS // TOK_EP)
    expert_ids = jax.vmap(lambda own, number: assign_block(jax.random.fold_in(key_list[1], 2), own, number, TOK_EP, EXPERTS, TOPK, C, 2))(expert_ids_keys, expert_ids_turns).reshape((TOKENS, TOPK))
    gate_scores = jnp.clip(0.05 + 0.55 * jax.random.uniform(key_list[2], (TOKENS, TOPK), jnp.float32) ** block_levels(key_list[2], (TOKENS, TOPK), ((0, 16),), -0.2, 0.2), 0.05, 0.6)
    routed_gate = bell_draw(key_list[3], (EXPERTS, D, FF), D ** -0.5, 0.078125, ((0, 16), (2, 2)))
    routed_up = bell_draw(key_list[4], (EXPERTS, D, FF), D ** -0.5, 0.078125, ((0, 16), (2, 2)))
    routed_down = noise_with(key_list[5], (EXPERTS, FF, D), FF ** -0.5, 0.1875, ((0, 16), (1, 2)), (1, 2, 2, 2.0))
    shared_gate = bell_draw(key_list[6], (D, FF_S), D ** -0.5, 0.078125, ((1, 2),))
    shared_up = bell_draw(key_list[7], (D, FF_S), D ** -0.5, 0.078125, ((1, 2),))
    shared_down = noise_with(key_list[8], (FF_S, D), FF_S ** -0.5, 0.1875, ((0, 2),), (0, 1, 2, 2.0))
    return {"tokens": tokens, "expert_ids": expert_ids, "gate_scores": gate_scores, "routed_gate": routed_gate, "routed_up": routed_up, "routed_down": routed_down, "shared_gate": shared_gate, "shared_up": shared_up, "shared_down": shared_down}


def routing(expert_ids, gate_scores, experts, capacity):
    row_count, top_count = expert_ids.shape
    entries = expert_ids.reshape(-1).astype(jnp.int32)
    onehot = (entries[:, None] == jnp.arange(experts, dtype=jnp.int32)[None, :]).astype(jnp.int32)
    before = jnp.cumsum(onehot, axis=0, dtype=jnp.int32) - onehot
    slot_rank = jnp.sum(before * onehot, axis=1).astype(jnp.int32)
    position = (entries * capacity + slot_rank).astype(jnp.int32)
    places = (jnp.arange(experts * capacity, dtype=jnp.int32)[:, None] == position[None, :])
    places = places.reshape(experts * capacity, row_count, top_count).astype(jnp.float32)
    select = jnp.sum(places, axis=2).astype(jnp.bfloat16)
    combine_weights = jnp.sum(places * gate_scores[None, :, :].astype(jnp.float32), axis=2)
    return select, combine_weights


def expert_pass(bucket_rows, w_gate, w_up, w_down):
    gate_sum = jnp.dot(bucket_rows, w_gate, preferred_element_type=jnp.float32)
    up_sum = jnp.dot(bucket_rows, w_up, preferred_element_type=jnp.float32)
    hidden = (jax.nn.silu(gate_sum) * up_sum).astype(jnp.bfloat16)
    row_count, hidden_width = hidden.shape
    group_width = hidden_width // N_TP
    hidden_groups = hidden.reshape(row_count, N_TP, group_width).transpose(1, 0, 2)
    down_groups = w_down.reshape(N_TP, group_width, w_down.shape[1])

    def add_group(total, pieces):
        partial_value = jnp.dot(pieces[0], pieces[1], preferred_element_type=jnp.float32)
        return total + partial_value.astype(jnp.bfloat16).astype(jnp.float32), None

    start = jnp.zeros((row_count, w_down.shape[1]), jnp.float32)
    total, unused = lax.scan(add_group, start, (hidden_groups, down_groups))
    return total


def reference(tokens, expert_ids, gate_scores, routed_gate, routed_up, routed_down, shared_gate, shared_up, shared_down):
    block_tokens = tokens.reshape(N_EP, TOK_EP, D)
    block_ids = expert_ids.reshape(N_EP, TOK_EP, TOPK)
    block_scores = gate_scores.reshape(N_EP, TOK_EP, TOPK)

    def fill_buckets(inputs):
        select, combine_weights = routing(inputs[1], inputs[2], EXPERTS, C)
        filled = jnp.dot(select, inputs[0], preferred_element_type=jnp.float32).astype(jnp.bfloat16)
        return filled, combine_weights

    buckets, weights = lax.map(fill_buckets, (block_tokens, block_ids, block_scores))
    by_expert = buckets.reshape(N_EP, EXPERTS, C, D).transpose(1, 0, 2, 3).reshape(EXPERTS, N_EP * C, D)

    def run_expert(inputs):
        return expert_pass(inputs[0], inputs[1], inputs[2], inputs[3]).astype(jnp.bfloat16)

    outputs = lax.map(run_expert, (by_expert, routed_gate, routed_up, routed_down))
    returned = outputs.reshape(EXPERTS, N_EP, C, D).transpose(1, 0, 2, 3).reshape(N_EP, EXPERTS * C, D)
    routed = jnp.einsum("spt,spd->std", weights, returned.astype(jnp.float32), precision=lax.Precision.HIGHEST)
    shared = expert_pass(tokens, shared_gate, shared_up, shared_down)
    return (routed.reshape(TOKENS, D) + shared).astype(jnp.bfloat16)
```

```python
import jax
import jax.numpy as jnp
from jax import lax
from jax.sharding import PartitionSpec as P


def routing(expert_ids, gate_scores, experts, capacity):
    row_count, top_count = expert_ids.shape
    entries = expert_ids.reshape(-1)
    onehot = (entries[:, None] == jnp.arange(experts, dtype=jnp.int32)[None, :]).astype(jnp.int32)
    before = jnp.cumsum(onehot, axis=0, dtype=jnp.int32) - onehot
    slot_rank = jnp.sum(before * onehot, axis=1)
    position = entries * capacity + slot_rank
    places = jnp.arange(experts * capacity, dtype=jnp.int32)[:, None] == position[None, :]
    places = places.reshape(experts * capacity, row_count, top_count).astype(jnp.float32)
    select = jnp.sum(places, axis=2).astype(jnp.bfloat16)
    combine_weights = jnp.sum(places * gate_scores[None, :, :], axis=2)
    return (select, combine_weights)


def fold_maker(w_gate, w_up, block_piece):
    return (
        jnp.dot(block_piece, w_gate, preferred_element_type=jnp.float32),
        jnp.dot(block_piece, w_up, preferred_element_type=jnp.float32),
    )


def bucketed(
    tokens,
    expert_ids,
    gate_scores,
    routed_gate,
    routed_up,
    routed_down,
    shared_gate,
    shared_up,
    shared_down,
):
    experts = routed_gate.shape[0] * lax.axis_size("ep")
    row_count, top_count = expert_ids.shape
    capacity = min(row_count, row_count * top_count * 15 // (8 * experts))
    select, combine_weights = routing(expert_ids, gate_scores, experts, capacity)
    width_local = tokens.shape[1]
    buckets = jnp.dot(select, tokens, preferred_element_type=jnp.float32).astype(jnp.bfloat16)
    buckets = buckets.reshape(experts, capacity, width_local)
    w_gate = routed_gate[0]
    w_up = routed_up[0]
    w_down = routed_down[0]
    shared_gate_sum, shared_up_sum = fold_maker(
        shared_gate, shared_up, lax.all_gather(tokens, "tp", axis=1, tiled=True)
    )
    shared_hidden = (jax.nn.silu(shared_gate_sum) * shared_up_sum).astype(jnp.bfloat16)
    shared_partial = jnp.dot(shared_hidden, shared_down, preferred_element_type=jnp.float32).astype(
        jnp.bfloat16
    )
    shared_out = lax.psum_scatter(shared_partial, "tp", scatter_dimension=1, tiled=True).astype(
        jnp.float32
    )
    received = lax.all_to_all(buckets, "ep", split_axis=0, concat_axis=0, tiled=True)
    gate_sum, up_sum = fold_maker(w_gate, w_up, lax.all_gather(received, "tp", axis=2, tiled=True))
    hidden = (jax.nn.silu(gate_sum) * up_sum).astype(jnp.bfloat16)
    partial_value = jnp.dot(hidden, w_down, preferred_element_type=jnp.float32).astype(jnp.bfloat16)
    summed = (
        lax.psum_scatter(partial_value, "tp", scatter_dimension=2, tiled=True)
        .astype(jnp.float32)
        .astype(jnp.bfloat16)
    )
    returned = lax.all_to_all(summed, "ep", split_axis=0, concat_axis=0, tiled=True)
    flat_returned = returned.reshape(experts * capacity, width_local).astype(jnp.float32)
    routed = jnp.einsum(
        "pt,pd->td", combine_weights, flat_returned, precision=lax.Precision.HIGHEST
    )
    return (routed + shared_out).astype(jnp.bfloat16)


def dense(
    tokens,
    expert_ids,
    gate_scores,
    routed_gate,
    routed_up,
    routed_down,
    shared_gate,
    shared_up,
    shared_down,
):
    ep, tp = lax.axis_size("ep"), lax.axis_size("tp")
    me = lax.axis_index("ep")
    rows, width = tokens.shape
    units = shared_gate.shape[1] // ep
    own = jnp.arange(ep, dtype=jnp.int32)
    scores = jnp.sum(
        jnp.where(expert_ids[:, :, None] == own[None, None, :], gate_scores[:, :, None], 0.0), axis=1
    )
    scores = lax.all_gather(scores, "ep", axis=0, tiled=True)
    weight = lax.dynamic_slice_in_dim(scores, me, 1, axis=1)
    held = lax.all_gather(tokens, ("ep", "tp"), axis=0, tiled=False).reshape(ep, tp, rows, width)
    features = [held[:, t].reshape(ep * rows, width) for t in range(tp)]
    s_gate = lax.dynamic_slice_in_dim(shared_gate, me * units, units, axis=1)
    s_up = lax.dynamic_slice_in_dim(shared_up, me * units, units, axis=1)
    s_down = lax.dynamic_slice_in_dim(shared_down, me * units, units, axis=0)

    def project(w):
        return sum(
            jnp.dot(
                features[t], w[t * width : (t + 1) * width], preferred_element_type=jnp.float32
            )
            for t in range(tp)
        )

    hidden = (jax.nn.silu(project(routed_gate[0])) * project(routed_up[0]) * weight).astype(
        jnp.bfloat16
    )
    s_hidden = (jax.nn.silu(project(s_gate)) * project(s_up)).astype(jnp.bfloat16)
    parts = []
    for t in range(tp):
        cut = slice(t * width, (t + 1) * width)
        part = jnp.dot(hidden, routed_down[0][:, cut], preferred_element_type=jnp.float32)
        part = part + jnp.dot(s_hidden, s_down[:, cut], preferred_element_type=jnp.float32)
        parts.append(part.astype(jnp.bfloat16).reshape(ep, 1, rows, width))
    partial = jnp.concatenate(parts, axis=1).reshape(ep * tp, rows, width)
    return lax.psum_scatter(partial, ("ep", "tp"), scatter_dimension=0, tiled=False)


def solution(mesh):
    placed = (
        P("ep", "tp"),
        P("ep", None),
        P("ep", None),
        P("ep", None, "tp"),
        P("ep", None, "tp"),
        P("ep", "tp", None),
        P(None, "tp"),
        P(None, "tp"),
        P("tp", None),
    )

    def local(*args):
        even = args[6].shape[1] % mesh.shape["ep"] == 0
        return (dense if even else bucketed)(*args)

    return jax.shard_map(
        local, mesh=mesh, in_specs=placed, out_specs=P("ep", "tp"), check_vma=False
    )
```

```python
import functools

import jax
import jax.numpy as jnp
from jax import lax
from jax.experimental import pallas as pl
from jax.experimental.pallas import tpu as pltpu
from jax.sharding import PartitionSpec as P


def routing(expert_ids, gate_scores, experts, capacity):
    row_count, top_count = expert_ids.shape
    entries = expert_ids.reshape(-1)
    onehot = (entries[:, None] == jnp.arange(experts, dtype=jnp.int32)[None, :]).astype(jnp.int32)
    before = jnp.cumsum(onehot, axis=0, dtype=jnp.int32) - onehot
    slot_rank = jnp.sum(before * onehot, axis=1)
    position = entries * capacity + slot_rank
    places = jnp.arange(experts * capacity, dtype=jnp.int32)[:, None] == position[None, :]
    places = places.reshape(experts * capacity, row_count, top_count).astype(jnp.float32)
    select = jnp.sum(places, axis=2).astype(jnp.bfloat16)
    combine_weights = jnp.sum(places * gate_scores[None, :, :], axis=2)
    return (select, combine_weights)


def fold_maker(w_gate, w_up, block_piece):
    return (
        jnp.dot(block_piece, w_gate, preferred_element_type=jnp.float32),
        jnp.dot(block_piece, w_up, preferred_element_type=jnp.float32),
    )


def bucketed(
    tokens,
    expert_ids,
    gate_scores,
    routed_gate,
    routed_up,
    routed_down,
    shared_gate,
    shared_up,
    shared_down,
):
    experts = routed_gate.shape[0] * lax.axis_size("ep")
    row_count, top_count = expert_ids.shape
    capacity = min(row_count, row_count * top_count * 15 // (8 * experts))
    select, combine_weights = routing(expert_ids, gate_scores, experts, capacity)
    width_local = tokens.shape[1]
    buckets = jnp.dot(select, tokens, preferred_element_type=jnp.float32).astype(jnp.bfloat16)
    buckets = buckets.reshape(experts, capacity, width_local)
    w_gate = routed_gate[0]
    w_up = routed_up[0]
    w_down = routed_down[0]
    shared_gate_sum, shared_up_sum = fold_maker(
        shared_gate, shared_up, lax.all_gather(tokens, "tp", axis=1, tiled=True)
    )
    shared_hidden = (jax.nn.silu(shared_gate_sum) * shared_up_sum).astype(jnp.bfloat16)
    shared_partial = jnp.dot(shared_hidden, shared_down, preferred_element_type=jnp.float32).astype(
        jnp.bfloat16
    )
    shared_out = lax.psum_scatter(shared_partial, "tp", scatter_dimension=1, tiled=True).astype(
        jnp.float32
    )
    received = lax.all_to_all(buckets, "ep", split_axis=0, concat_axis=0, tiled=True)
    gate_sum, up_sum = fold_maker(w_gate, w_up, lax.all_gather(received, "tp", axis=2, tiled=True))
    hidden = (jax.nn.silu(gate_sum) * up_sum).astype(jnp.bfloat16)
    partial_value = jnp.dot(hidden, w_down, preferred_element_type=jnp.float32).astype(jnp.bfloat16)
    summed = (
        lax.psum_scatter(partial_value, "tp", scatter_dimension=2, tiled=True)
        .astype(jnp.float32)
        .astype(jnp.bfloat16)
    )
    returned = lax.all_to_all(summed, "ep", split_axis=0, concat_axis=0, tiled=True)
    flat_returned = returned.reshape(experts * capacity, width_local).astype(jnp.float32)
    routed = jnp.einsum(
        "pt,pd->td", combine_weights, flat_returned, precision=lax.Precision.HIGHEST
    )
    return (routed + shared_out).astype(jnp.bfloat16)


LANES = 128
TILE = 256
QUAD = 4
MESH = pl.DeviceIdType.MESH


def layer_kernel(
    ep,
    x_ref,
    gate_hbm,
    up_hbm,
    down_hbm,
    s_in_hbm,
    s_down_hbm,
    out_ref,
    xbuf,
    w_gate,
    w_up,
    w_down,
    w_shared,
    hidden,
    mine,
    other,
    other_in,
    last_in,
    line_in,
    first_in,
    w_sem,
    own_sem,
    gather_send,
    gather_recv,
    core_send,
    core_recv,
    last_send,
    last_recv,
    line_send,
    line_recv,
    first_send,
    first_recv,
):
    depth = ep // QUAD
    rows, width = out_ref.shape
    units = w_gate.shape[1]
    e, c = lax.axis_index("ep"), lax.axis_index("tp")
    z, y, x = e // QUAD, (e // 2) % 2, e % 2
    flip_x, flip_y = 1 - 2 * x, 1 - 2 * y
    f = x * (1 - c) + y * c
    l = y * (1 - c) + x * c

    def block(zz, ff, ll):
        return zz * QUAD + (1 - c) * (2 * ll + ff) + c * (2 * ff + ll)

    sibling = (e, 1 - c)
    first = (e + (1 - c) * flip_x + c * 2 * flip_y, c)
    last = (e + c * flip_x + (1 - c) * 2 * flip_y, c)
    above = (e + QUAD, c)
    below = (e - QUAD, c)
    has_above, has_below = z < depth - 1, z > 0

    loads = [
        pltpu.make_async_copy(gate_hbm, w_gate, w_sem.at[0]),
        pltpu.make_async_copy(up_hbm, w_up, w_sem.at[1]),
        pltpu.make_async_copy(s_in_hbm, w_shared, w_sem.at[2]),
        pltpu.make_async_copy(down_hbm, w_down.at[pl.ds(0, units)], w_sem.at[3]),
        pltpu.make_async_copy(
            s_down_hbm, w_down.at[pl.ds(units, s_down_hbm.shape[0])], w_sem.at[4]
        ),
    ]
    own = pltpu.make_async_copy(x_ref, xbuf.at[c, e], own_sem)
    own.start()
    for load in loads:
        load.start()

    barrier = pltpu.get_barrier_semaphore()
    for peer in (sibling, first, last):
        pl.semaphore_signal(barrier, inc=1, device_id=peer, device_id_type=MESH)

    @pl.when(has_above)
    def _():
        pl.semaphore_signal(barrier, inc=1, device_id=above, device_id_type=MESH)

    @pl.when(has_below)
    def _():
        pl.semaphore_signal(barrier, inc=1, device_id=below, device_id_type=MESH)

    pl.semaphore_wait(
        barrier, 3 + jnp.where(has_above, 1, 0) + jnp.where(has_below, 1, 0)
    )
    own.wait()

    def gather_copy(kind, b, half, peer):
        return pltpu.make_async_remote_copy(
            src_ref=xbuf.at[half, b],
            dst_ref=xbuf.at[half, b],
            send_sem=gather_send.at[kind, b],
            recv_sem=gather_recv.at[half, b],
            device_id=peer,
            device_id_type=MESH,
        )

    TO_FIRST, TO_LAST, TO_ABOVE, TO_BELOW, TO_CORE = range(5)

    def arrived(b, half):
        gather_copy(TO_CORE, b, half, sibling).wait_recv()

    def up_down(b, go_above, go_below):
        @pl.when(go_above)
        def _():
            gather_copy(TO_ABOVE, b, c, above).start()

        @pl.when(go_below)
        def _():
            gather_copy(TO_BELOW, b, c, below).start()

    gather_copy(TO_FIRST, e, c, first).start()
    up_down(e, has_above, has_below)
    gather_copy(TO_LAST, e, c, last).start()
    gather_copy(TO_CORE, e, c, sibling).start()
    partner = block(z, 1 - f, l)
    arrived(partner, c)
    up_down(partner, has_above, has_below)
    gather_copy(TO_LAST, partner, c, last).start()
    gather_copy(TO_CORE, partner, c, sibling).start()

    def from_last(zz):
        for ff in range(2):
            b = block(zz, ff, 1 - l)
            arrived(b, c)
            gather_copy(TO_CORE, b, c, sibling).start()

    for d in range(1, depth):
        for ff in (f, 1 - f):

            @pl.when(z - d >= 0)
            def _():
                b = block(z - d, ff, l)
                arrived(b, c)
                up_down(b, has_above, False)
                gather_copy(TO_LAST, b, c, last).start()
                gather_copy(TO_CORE, b, c, sibling).start()

            @pl.when(z + d < depth)
            def _():
                b = block(z + d, ff, l)
                arrived(b, c)
                up_down(b, False, has_below)
                gather_copy(TO_LAST, b, c, last).start()
                gather_copy(TO_CORE, b, c, sibling).start()

        if d == 1:
            from_last(z)
        else:
            pl.when(z - d + 1 >= 0)(lambda: from_last(z - d + 1))
            pl.when(z + d - 1 < depth)(lambda: from_last(z + d - 1))
    pl.when(z - depth + 1 >= 0)(lambda: from_last(z - depth + 1))
    pl.when(z + depth - 1 < depth)(lambda: from_last(z + depth - 1))

    @pl.loop(0, ep)
    def _(b):
        arrived(b, 1 - c)

    for load in loads[:3]:
        load.wait()

    tokens = ep * rows
    tag = xbuf[0, :, :, pl.ds(width, LANES)].reshape(tokens, LANES).astype(jnp.float32)
    lane = lax.broadcasted_iota(jnp.int32, (tokens, LANES), 1)
    chosen = (lane == e) | (lane == e + ep) | (lane == e + 2 * ep)
    weight = jnp.sum(jnp.where(chosen, tag, 0.0), axis=1, keepdims=True)

    def project(w_ref, start):
        total = None
        for half in range(2):
            part = jnp.dot(
                xbuf[half, :, :, pl.ds(0, width)].reshape(tokens, width),
                w_ref[pl.ds(half * width, width), pl.ds(start, TILE)],
                preferred_element_type=jnp.float32,
            )
            total = part if total is None else total + part
        return total

    @pl.loop(0, units // TILE)
    def _(j):
        start = pl.multiple_of(j * TILE, TILE)
        g = project(w_gate, start)
        u = project(w_up, start)
        h = g / (1.0 + jnp.exp(-g)) * u * weight
        hidden[:, pl.ds(start, TILE)] = h.astype(jnp.bfloat16)

    both = project(w_shared, 0)
    g, u = both[:, :LANES], both[:, LANES:]
    hidden[:, pl.ds(units, LANES)] = (g / (1.0 + jnp.exp(-g)) * u).astype(jnp.bfloat16)

    for load in loads[3:]:
        load.wait()

    def contract(half, target):
        @pl.loop(0, width // TILE)
        def _(j):
            start = pl.multiple_of(j * TILE, TILE)
            column = pl.multiple_of(half * width + j * TILE, TILE)
            part = jnp.dot(
                hidden[...], w_down[:, pl.ds(column, TILE)], preferred_element_type=jnp.float32
            )
            target[:, :, pl.ds(start, TILE)] = part.astype(jnp.bfloat16).reshape(ep, rows, TILE)

    contract(1 - c, other)
    to_core = pltpu.make_async_remote_copy(
        src_ref=other,
        dst_ref=other_in,
        send_sem=core_send,
        recv_sem=core_recv,
        device_id=sibling,
        device_id_type=MESH,
    )
    to_core.start()
    contract(c, mine)
    to_core.wait()

    def add(b, ref, *at):
        mine[b] = (mine[b].astype(jnp.float32) + ref[at].astype(jnp.float32)).astype(jnp.bfloat16)

    order = []
    for zz in range(depth):
        near = sorted(range(depth), key=lambda p: (-abs(p - zz), p))
        order.append(near)

    def pick(k):
        p = jnp.int32(0)
        for zz in range(depth):
            p = jnp.where(z == zz, order[zz][k], p)
        return p

    def last_copy(p, ff, b):
        return pltpu.make_async_remote_copy(
            src_ref=mine.at[b],
            dst_ref=last_in.at[p, ff],
            send_sem=last_send.at[p, ff],
            recv_sem=last_recv.at[p, ff],
            device_id=last,
            device_id_type=MESH,
        )

    def line_copy(p, ff, b, slot, peer):
        return pltpu.make_async_remote_copy(
            src_ref=mine.at[b],
            dst_ref=line_in.at[slot, ff],
            send_sem=line_send.at[p, ff],
            recv_sem=line_recv.at[slot, ff],
            device_id=peer,
            device_id_type=MESH,
        )

    for k in range(depth):
        p = pick(k)
        for ff in range(2):
            b = block(p, ff, 1 - l)
            add(b, other_in, b)
            last_copy(p, ff, b).start()

    home = block(z, 1 - f, l)
    to_first = pltpu.make_async_remote_copy(
        src_ref=mine.at[home],
        dst_ref=first_in,
        send_sem=first_send,
        recv_sem=first_recv,
        device_id=first,
        device_id_type=MESH,
    )
    for k in range(depth):
        p = pick(k)
        for ff in (1 - f, f):
            b = block(p, ff, l)
            add(b, other_in, b)
            last_copy(p, ff, b).wait_recv()
            add(b, last_in, p, ff)

            @pl.when((p >= z) & has_below)
            def _():
                line_copy(p, ff, b, p, above).wait_recv()
                add(b, line_in, p, ff)

            @pl.when((p <= z) & has_above)
            def _():
                slot = jnp.where(p == z, depth, p)
                line_copy(p, ff, b, slot, below).wait_recv()
                add(b, line_in, slot, ff)

            @pl.when(p > z)
            def _():
                line_copy(p, ff, b, p, above).start()

            @pl.when(p < z)
            def _():
                slot = jnp.where(p == z - 1, depth, p)
                line_copy(p, ff, b, slot, below).start()

        if k == depth - 1:
            to_first.start()

    to_first.wait()
    out_ref[...] = (mine[e].astype(jnp.float32) + first_in[...].astype(jnp.float32)).astype(
        jnp.bfloat16
    )

    for p in range(depth):
        for ff in range(2):
            last_copy(p, ff, block(p, ff, 1 - l)).wait_send()

            @pl.when(p != z)
            def _():
                line_copy(p, ff, block(p, ff, l), p, above).wait_send()

    gather_copy(TO_FIRST, e, c, first).wait_send()
    for zz in range(depth):
        for ff in range(2):
            b = block(zz, ff, l)
            gather_copy(TO_LAST, b, c, last).wait_send()
            pl.when((zz <= z) & has_above)(
                lambda: gather_copy(TO_ABOVE, b, c, above).wait_send()
            )
            pl.when((zz >= z) & has_below)(
                lambda: gather_copy(TO_BELOW, b, c, below).wait_send()
            )

    @pl.loop(0, ep)
    def _(b):
        gather_copy(TO_CORE, b, c, sibling).wait_send()


def dense(
    tokens,
    expert_ids,
    gate_scores,
    routed_gate,
    routed_up,
    routed_down,
    shared_gate,
    shared_up,
    shared_down,
):
    ep = lax.axis_size("ep")
    me = lax.axis_index("ep")
    rows, width = tokens.shape
    depth = ep // QUAD
    features, units = routed_gate.shape[1:]
    share = shared_gate.shape[1] // ep
    spare = LANES - share
    own = jnp.arange(ep, dtype=jnp.int32)
    scores = jnp.sum(
        jnp.where(expert_ids[:, :, None] == own[None, None, :], gate_scores[:, :, None], 0.0), axis=1
    )
    high = lax.reduce_precision(scores, 8, 7)
    middle = lax.reduce_precision(scores - high, 8, 7)
    low = scores - high - middle
    tag = jnp.concatenate([high, middle, low], axis=1).astype(jnp.bfloat16)
    tagged = jnp.concatenate(
        [tokens, jnp.pad(tag, ((0, 0), (0, LANES - tag.shape[1])))], axis=1
    )
    s_gate = lax.dynamic_slice_in_dim(shared_gate, me * share, share, axis=1)
    s_up = lax.dynamic_slice_in_dim(shared_up, me * share, share, axis=1)
    s_in = jnp.concatenate(
        [jnp.pad(s_gate, ((0, 0), (0, spare))), jnp.pad(s_up, ((0, 0), (0, spare)))], axis=1
    )
    s_down = jnp.pad(
        lax.dynamic_slice_in_dim(shared_down, me * share, share, axis=0), ((0, spare), (0, 0))
    )
    vmem = pl.BlockSpec(memory_space=pltpu.VMEM)
    far = pl.BlockSpec(memory_space=pl.ANY)
    half = (rows, width)
    dtype = tokens.dtype
    dma = pltpu.SemaphoreType.DMA
    return pl.pallas_call(
        functools.partial(layer_kernel, ep),
        out_shape=jax.ShapeDtypeStruct(half, dtype),
        in_specs=[vmem] + [far] * 5,
        out_specs=vmem,
        scratch_shapes=[
            pltpu.VMEM((2, ep, rows, width + LANES), dtype),
            pltpu.VMEM((features, units), dtype),
            pltpu.VMEM((features, units), dtype),
            pltpu.VMEM((units + LANES, features), dtype),
            pltpu.VMEM((features, TILE), dtype),
            pltpu.VMEM((ep * rows, units + LANES), dtype),
            pltpu.VMEM((ep,) + half, dtype),
            pltpu.VMEM((ep,) + half, dtype),
            pltpu.VMEM((ep,) + half, dtype),
            pltpu.VMEM((depth, 2) + half, dtype),
            pltpu.VMEM((depth + 1, 2) + half, dtype),
            pltpu.VMEM(half, dtype),
            dma((5,)),
            dma,
            dma((5, ep)),
            dma((2, ep)),
            dma,
            dma,
            dma((depth, 2)),
            dma((depth, 2)),
            dma((depth, 2)),
            dma((depth + 1, 2)),
            dma,
            dma,
        ],
        compiler_params=pltpu.CompilerParams(
            collective_id=0, has_side_effects=True, vmem_limit_bytes=67043328
        ),
    )(tagged, routed_gate[0], routed_up[0], routed_down[0], s_in, s_down)


def solution(mesh):
    placed = (
        P("ep", "tp"),
        P("ep", None),
        P("ep", None),
        P("ep", None, "tp"),
        P("ep", None, "tp"),
        P("ep", "tp", None),
        P(None, "tp"),
        P(None, "tp"),
        P("tp", None),
    )

    def local(*args):
        ep, tp = mesh.shape["ep"], mesh.shape["tp"]
        fits = tp == 2 and ep == QUAD * QUAD and args[6].shape[1] % ep == 0
        return (dense if fits else bucketed)(*args)

    return jax.shard_map(
        local, mesh=mesh, in_specs=placed, out_specs=P("ep", "tp"), check_vma=False
    )
```
